32 devices in a mesh: tp: 4 (over z), fsdp: 8 (over y, x, core).
Axes of the slice: x: 2, y: 2, z: 4, core: 2. Of those that a mesh axis runs over, the one named last changes fastest.
Arguments:
- resid_in: bfloat16 [8, 1536, 5120], P('fsdp', 'tp')
- grad_out: bfloat16 [8, 1536, 5120], P('fsdp', 'tp')
- norm_gain: float32 [5120], replicated
- w_qkv: bfloat16 [5120, 7168], P('fsdp', 'tp')
- b_qkv: bfloat16 [7168], P('tp')
- sinks: float32 [40], P('tp')
- w_out: bfloat16 [5120, 5120], P(('tp', 'fsdp'))
- b_out: bfloat16 [5120], replicated
Outputs:
- output 1: bfloat16 [8, 1536, 5120], P('fsdp', 'tp')
- output 2: bfloat16 [8, 1536, 5120], P('fsdp', 'tp')
- output 3: float32 [5120], replicated
- output 4: float32 [5120, 7168], P('fsdp', 'tp')
- output 5: float32 [7168], P('tp')
- output 6: float32 [40], P('tp')
- output 7: float32 [5120, 5120], P(('tp', 'fsdp'))
- output 8: float32 [5120], replicated
All inputs are finite; a program needn't handle non-finite values.
Results may differ from the reference program's by a relative error of at most 0.0108997.
Values are sent between devices in bfloat16 or wider.
A program may use at most 1 GiB of HBM per device.

```python
import jax
import jax.numpy as jnp
from jax import lax

D = 5120
HEADS = 40
KV_HEADS = 8
HEAD = 128
WINDOW = 128
BATCH = 8
SEQ = 1536

GROUP = HEADS // KV_HEADS
QKV_COLS = (HEADS + 2 * KV_HEADS) * HEAD
N_BLOCKS = SEQ // WINDOW
EPS = 1e-5
ROPE_BASE = 150000.0


def setup_inputs(seed: int = 0) -> dict:
    rng_keys = jax.random.split(jax.random.key(seed), 8)
    resid_in = jax.random.normal(rng_keys[0], (BATCH, SEQ, D), jnp.float32)
    grad_out = jax.random.normal(rng_keys[1], (BATCH, SEQ, D), jnp.float32)
    norm_gain = 1.0 + 0.3 * jax.random.normal(rng_keys[2], (D,), jnp.float32)
    w_qkv = (1.2 / D ** 0.5) * jax.random.normal(rng_keys[3], (D, QKV_COLS), jnp.float32)
    b_qkv = 0.5 * jax.random.normal(rng_keys[4], (QKV_COLS,), jnp.float32)
    sinks = 5.0 + 1.5 * jax.random.normal(rng_keys[5], (HEADS,), jnp.float32)
    w_out = (1.5 / (HEADS * HEAD) ** 0.5) * jax.random.normal(rng_keys[6], (HEADS * HEAD, D), jnp.float32)
    b_out = 0.5 * jax.random.normal(rng_keys[7], (D,), jnp.float32)
    return {
        "resid_in": resid_in.astype(jnp.bfloat16),
        "grad_out": grad_out.astype(jnp.bfloat16),
        "norm_gain": norm_gain,
        "w_qkv": w_qkv.astype(jnp.bfloat16),
        "b_qkv": b_qkv.astype(jnp.bfloat16),
        "sinks": sinks,
        "w_out": w_out.astype(jnp.bfloat16),
        "b_out": b_out.astype(jnp.bfloat16),
    }


def rope_tables(length):
    positions = jnp.arange(length).astype(jnp.float32)
    inv_freq = ROPE_BASE ** (-2.0 * jnp.arange(HEAD // 2).astype(jnp.float32) / HEAD)
    angles = positions[:, None] * inv_freq[None, :]
    return jnp.cos(angles), jnp.sin(angles)


def apply_rope(head_vals, cos_tab, sin_tab):
    half_dim = head_vals.shape[-1] // 2
    first_half = head_vals[..., :half_dim]
    second_half = head_vals[..., half_dim:]
    return jnp.concatenate([first_half * cos_tab - second_half * sin_tab, second_half * cos_tab + first_half * sin_tab], axis=-1)


def block_attend(block_in, sinks):
    q_blk, k_blk, v_blk, block_idx = block_in
    scores = jnp.einsum("iegd,jed->egij", q_blk, k_blk) / HEAD ** 0.5
    q_idx = jnp.arange(WINDOW)[:, None]
    k_idx = jnp.arange(2 * WINDOW)[None, :]
    allowed = (k_idx > q_idx) & (k_idx <= q_idx + WINDOW) & (block_idx * WINDOW - WINDOW + k_idx >= 0)
    scores = jnp.where(allowed, scores, -1e30)
    sink_col = sinks.reshape(KV_HEADS, GROUP)[:, :, None, None]
    row_max = lax.stop_gradient(jnp.maximum(jnp.max(scores, axis=-1, keepdims=True), sink_col))
    exp_scores = jnp.exp(scores - row_max)
    row_denom = jnp.sum(exp_scores, axis=-1, keepdims=True) + jnp.exp(sink_col - row_max)
    attn_probs = (exp_scores / row_denom).astype(jnp.bfloat16).astype(jnp.float32)
    return jnp.einsum("egij,jed->iegd", attn_probs, v_blk)


def row_forward(resid_row, params):
    norm_gain, w_qkv, b_qkv, sinks, w_out, b_out = params
    mean_sq = jnp.mean(resid_row * resid_row, axis=-1, keepdims=True)
    normed = (resid_row * lax.rsqrt(mean_sq + EPS) * norm_gain).astype(jnp.bfloat16).astype(jnp.float32)
    qkv_proj = (jnp.dot(normed, w_qkv, preferred_element_type=jnp.float32) + b_qkv).astype(jnp.bfloat16).astype(jnp.float32)
    qkv_proj = qkv_proj.reshape(SEQ, KV_HEADS, GROUP + 2, HEAD)
    cos_tab, sin_tab = rope_tables(SEQ)
    queries = apply_rope(qkv_proj[:, :, :GROUP], cos_tab[:, None, None], sin_tab[:, None, None]).astype(jnp.bfloat16).astype(jnp.float32)
    keys_rot = apply_rope(qkv_proj[:, :, GROUP], cos_tab[:, None], sin_tab[:, None]).astype(jnp.bfloat16).astype(jnp.float32)
    values = qkv_proj[:, :, GROUP + 1]
    zero_pad = jnp.zeros((WINDOW, KV_HEADS, HEAD), jnp.float32)
    k_prev = jnp.concatenate([zero_pad, keys_rot[:SEQ - WINDOW]], axis=0).reshape(N_BLOCKS, WINDOW, KV_HEADS, HEAD)
    v_prev = jnp.concatenate([zero_pad, values[:SEQ - WINDOW]], axis=0).reshape(N_BLOCKS, WINDOW, KV_HEADS, HEAD)
    k_blocks = jnp.concatenate([k_prev, keys_rot.reshape(N_BLOCKS, WINDOW, KV_HEADS, HEAD)], axis=1)
    v_blocks = jnp.concatenate([v_prev, values.reshape(N_BLOCKS, WINDOW, KV_HEADS, HEAD)], axis=1)
    q_blocks = queries.reshape(N_BLOCKS, WINDOW, KV_HEADS, GROUP, HEAD)
    attend = jax.checkpoint(block_attend)
    attn_out = lax.map(lambda block_in: attend(block_in, sinks), (q_blocks, k_blocks, v_blocks, jnp.arange(N_BLOCKS)))
    attn_out = attn_out.reshape(SEQ, HEADS * HEAD).astype(jnp.bfloat16).astype(jnp.float32)
    resid_out = resid_row + jnp.dot(attn_out, w_out, preferred_element_type=jnp.float32) + b_out
    return resid_out.astype(jnp.bfloat16)


def reference(resid_in, grad_out, norm_gain, w_qkv, b_qkv, sinks, w_out, b_out):
    params = (norm_gain, w_qkv.astype(jnp.float32), b_qkv.astype(jnp.float32), sinks, w_out.astype(jnp.float32), b_out.astype(jnp.float32))

    def row_step(grad_acc, row_in):
        resid_row, grad_row = row_in
        resid_out, pullback = jax.vjp(row_forward, resid_row.astype(jnp.float32), params)
        d_resid, row_grads = pullback(grad_row)
        new_acc = tuple(acc_sum + new_grad for acc_sum, new_grad in zip(grad_acc, row_grads))
        return new_acc, (resid_out, d_resid.astype(jnp.bfloat16))

    zero_acc = tuple(jnp.zeros_like(param_val) for param_val in params)
    grad_sums, (resid_rows, grad_rows) = lax.scan(row_step, zero_acc, (resid_in, grad_out))
    return (resid_rows, grad_rows, grad_sums[0], grad_sums[1], grad_sums[2], grad_sums[3], grad_sums[4], grad_sums[5])
```

```python
import jax
import jax.numpy as jnp
from jax import lax
from jax.sharding import PartitionSpec as P


EPS = 1e-5
ROPE_BASE = 150000.0
WINDOW = 128


def rope_tables(positions, head_dim):
    inv_freq = ROPE_BASE ** (-2.0 * jnp.arange(head_dim // 2).astype(jnp.float32) / head_dim)
    angles = positions.astype(jnp.float32)[:, None] * inv_freq[None, :]
    return jnp.cos(angles), jnp.sin(angles)


def apply_rope(head_vals, cos_tab, sin_tab):
    half_dim = head_vals.shape[-1] // 2
    first_half = head_vals[..., :half_dim]
    second_half = head_vals[..., half_dim:]
    return jnp.concatenate([first_half * cos_tab - second_half * sin_tab, second_half * cos_tab + first_half * sin_tab], axis=-1)


def rope_back(head_grads, cos_tab, sin_tab):
    half_dim = head_grads.shape[-1] // 2
    first_half = head_grads[..., :half_dim]
    second_half = head_grads[..., half_dim:]
    return jnp.concatenate([first_half * cos_tab + second_half * sin_tab, second_half * cos_tab - first_half * sin_tab], axis=-1)


def split_qkv(qkv_proj, positions, kv_count, head_dim):
    n_rows, seq_len = qkv_proj.shape[0], qkv_proj.shape[1]
    grouped = qkv_proj.reshape(n_rows, seq_len, kv_count, -1, head_dim)
    group_size = grouped.shape[3] - 2
    cos_tab, sin_tab = rope_tables(positions, head_dim)
    queries = apply_rope(grouped[:, :, :, :group_size].astype(jnp.float32), cos_tab[:, None, None], sin_tab[:, None, None])
    keys_rot = apply_rope(grouped[:, :, :, group_size].astype(jnp.float32), cos_tab[:, None], sin_tab[:, None])
    return queries.astype(jnp.bfloat16), keys_rot.astype(jnp.bfloat16), grouped[:, :, :, group_size + 1]


def band_mask(first_pos, blk_start):
    q_idx = jnp.arange(WINDOW)[:, None]
    k_idx = jnp.arange(2 * WINDOW)[None, :]
    return (k_idx > q_idx) & (k_idx <= q_idx + WINDOW) & (first_pos + blk_start - WINDOW + k_idx >= 0)


def block_scores(q_blk, k_blk, first_pos, blk_start):
    qk_scale = q_blk.shape[-1] ** -0.5
    scores = jnp.einsum("niegd,njed->negij", q_blk, k_blk, preferred_element_type=jnp.float32) * qk_scale
    return jnp.where(band_mask(first_pos, blk_start), scores, -1e30)


def attend_forward(queries, keys_ext, values_ext, sink_loc, first_pos):
    n_rows, q_len, kv_loc, group_size, _ = queries.shape
    sink_col = sink_loc.reshape(1, kv_loc, group_size, 1)

    def block_body(block_idx, loop_carry):
        out_acc, norm_acc = loop_carry
        blk_start = block_idx * WINDOW
        q_blk = lax.dynamic_slice_in_dim(queries, blk_start, WINDOW, axis=1)
        k_blk = lax.dynamic_slice_in_dim(keys_ext, blk_start, 2 * WINDOW, axis=1)
        v_blk = lax.dynamic_slice_in_dim(values_ext, blk_start, 2 * WINDOW, axis=1)
        scores = block_scores(q_blk, k_blk, first_pos, blk_start)
        row_max = jnp.maximum(jnp.max(scores, axis=-1), sink_col)
        exp_scores = jnp.exp(scores - row_max[..., None])
        row_denom = jnp.sum(exp_scores, axis=-1) + jnp.exp(sink_col - row_max)
        attn_probs = (exp_scores / row_denom[..., None]).astype(jnp.bfloat16)
        out_blk = jnp.einsum("negij,njed->niegd", attn_probs, v_blk, preferred_element_type=jnp.float32)
        out_acc = lax.dynamic_update_slice_in_dim(out_acc, out_blk.astype(jnp.bfloat16), blk_start, axis=1)
        norm_acc = lax.dynamic_update_slice_in_dim(norm_acc, row_max + jnp.log(row_denom), blk_start, axis=3)
        return out_acc, norm_acc

    init_carry = (jnp.zeros(queries.shape, jnp.bfloat16), jnp.zeros((n_rows, kv_loc, group_size, q_len), jnp.float32))
    return lax.fori_loop(0, q_len // WINDOW, block_body, init_carry)


def attend_backward(queries, keys_ext, values_ext, sink_loc, first_pos, log_norm, d_out):
    _, q_len, kv_loc, group_size, head_dim = queries.shape
    qk_scale = head_dim ** -0.5
    sink_col = sink_loc.reshape(1, kv_loc, group_size, 1)

    def block_body(block_idx, loop_carry):
        dq_acc, dk_acc, dv_acc, dsink_acc = loop_carry
        blk_start = block_idx * WINDOW
        q_blk = lax.dynamic_slice_in_dim(queries, blk_start, WINDOW, axis=1)
        k_blk = lax.dynamic_slice_in_dim(keys_ext, blk_start, 2 * WINDOW, axis=1)
        v_blk = lax.dynamic_slice_in_dim(values_ext, blk_start, 2 * WINDOW, axis=1)
        do_blk = lax.dynamic_slice_in_dim(d_out, blk_start, WINDOW, axis=1)
        norm_blk = lax.dynamic_slice_in_dim(log_norm, blk_start, WINDOW, axis=3)
        attn_probs = jnp.exp(block_scores(q_blk, k_blk, first_pos, blk_start) - norm_blk[..., None])
        dv_blk = jnp.einsum("negij,niegd->njed", attn_probs.astype(jnp.bfloat16), do_blk, preferred_element_type=jnp.float32)
        d_probs = jnp.einsum("niegd,njed->negij", do_blk, v_blk, preferred_element_type=jnp.float32).astype(jnp.bfloat16).astype(jnp.float32)
        row_dot = jnp.sum(attn_probs * d_probs, axis=-1)
        d_scores = (attn_probs * (d_probs - row_dot[..., None])).astype(jnp.bfloat16)
        sink_probs = jnp.exp(sink_col - norm_blk)
        dsink_acc = dsink_acc - jnp.sum(sink_probs * row_dot, axis=(0, 3))
        dq_blk = jnp.einsum("negij,njed->niegd", d_scores, k_blk, preferred_element_type=jnp.float32) * qk_scale
        dk_blk = jnp.einsum("negij,niegd->njed", d_scores, q_blk, preferred_element_type=jnp.float32) * qk_scale
        dq_acc = lax.dynamic_update_slice_in_dim(dq_acc, dq_blk.astype(jnp.bfloat16), blk_start, axis=1)
        dk_acc = lax.dynamic_update_slice_in_dim(dk_acc, lax.dynamic_slice_in_dim(dk_acc, blk_start, 2 * WINDOW, axis=1) + dk_blk, blk_start, axis=1)
        dv_acc = lax.dynamic_update_slice_in_dim(dv_acc, lax.dynamic_slice_in_dim(dv_acc, blk_start, 2 * WINDOW, axis=1) + dv_blk, blk_start, axis=1)
        return dq_acc, dk_acc, dv_acc, dsink_acc

    init_carry = (jnp.zeros(queries.shape, jnp.bfloat16), jnp.zeros(keys_ext.shape, jnp.float32), jnp.zeros(values_ext.shape, jnp.float32), jnp.zeros((kv_loc, group_size), jnp.float32))
    dq_all, dk_all, dv_all, dsink_all = lax.fori_loop(0, q_len // WINDOW, block_body, init_carry)
    return dq_all, dk_all, dv_all, dsink_all.reshape(-1)


def norm_backward(d_normed, resid_f32, inv_rms, norm_gain, grad_loc):
    d_normed = d_normed.astype(jnp.bfloat16).astype(jnp.float32)
    gain_grad = d_normed * norm_gain
    d_resid = inv_rms * (gain_grad - resid_f32 * inv_rms * inv_rms * jnp.mean(gain_grad * resid_f32, axis=-1, keepdims=True))
    grad_resid = (grad_loc.astype(jnp.float32) + d_resid).astype(jnp.bfloat16)
    grad_gain = jnp.sum(d_normed * resid_f32 * inv_rms, axis=(0, 1))
    return grad_resid, grad_gain


def ordered(value, *earlier):
    return lax.optimization_barrier((value, earlier))[0]


def tp_shift(value, step, n_ranks):
    return lax.ppermute(value, "tp", [(rank, (rank + step) % n_ranks) for rank in range(n_ranks)])


def ring_gather(shard, n_ranks, *earlier):
    pieces = [shard]
    held = ordered(shard, *earlier) if earlier else shard
    for _ in range(n_ranks - 1):
        held = tp_shift(held, 1, n_ranks)
        pieces.append(held)
    return pieces


def exchange(pieces_by_dest, n_ranks):
    received = [pieces_by_dest[0]]
    for step in range(1, n_ranks):
        received.append(tp_shift(pieces_by_dest[step], step, n_ranks))
    return received


def solution(mesh):
    act_spec = P("fsdp", "tp", None)
    wout_spec = P(("tp", "fsdp"), None)
    in_specs = (act_spec, act_spec, P(), P("fsdp", "tp"), P("tp"), P("tp"), wout_spec, P())
    out_specs = (act_spec, act_spec, P(), P("fsdp", "tp"), P("tp"), P("tp"), wout_spec, P())
    n_tp = mesh.shape["tp"]
    n_fsdp = mesh.shape["fsdp"]

    def device_step(resid_loc, grad_loc, norm_gain, wqkv_loc, bqkv_loc, sink_loc, wout_loc, b_out):
        n_rows, loc_len, _ = resid_loc.shape
        heads_loc = sink_loc.shape[0]
        rank = lax.axis_index("tp")
        seq_len = loc_len * n_tp
        head_dim = wout_loc.shape[0] * n_fsdp // heads_loc
        kv_loc = (wqkv_loc.shape[1] // head_dim - heads_loc) // 2
        out_loc = heads_loc * head_dim

        def chunk_of(arr, owner):
            return lax.dynamic_slice_in_dim(arr, lax.rem(owner + n_tp, n_tp) * loc_len, loc_len, axis=1)

        def to_sequence(pieces):
            out = jnp.zeros((n_rows, seq_len) + pieces[0].shape[2:], pieces[0].dtype)
            for step, piece in enumerate(pieces):
                out = lax.dynamic_update_slice_in_dim(out, piece, lax.rem(rank - step + n_tp, n_tp) * loc_len, axis=1)
            return out

        resid_f32 = resid_loc.astype(jnp.float32)
        inv_rms = lax.rsqrt(jnp.mean(resid_f32 * resid_f32, axis=-1, keepdims=True) + EPS)
        normed = (resid_f32 * inv_rms * norm_gain).astype(jnp.bfloat16)

        wqkv_own = lax.all_gather(wqkv_loc, "fsdp", axis=0, tiled=True)
        wout_ring = ring_gather(wout_loc, n_tp)
        wout_all = lax.all_gather(jnp.concatenate(wout_ring, axis=0), "fsdp", axis=0, tiled=True)

        def project(piece):
            return (jnp.dot(piece, wqkv_own, preferred_element_type=jnp.float32) + bqkv_loc.astype(jnp.float32)).astype(jnp.bfloat16)

        d_attn_rows = jnp.einsum("ntk,hk->nth", grad_loc, wout_all, preferred_element_type=jnp.float32).astype(jnp.bfloat16)
        d_attn_rows = d_attn_rows.reshape(n_rows, loc_len, n_fsdp, n_tp, -1)
        d_attn_send = [d_attn_rows[:, :, :, (n_tp - step) % n_tp].reshape(n_rows, loc_len, out_loc) for step in range(n_tp)]

        normed_ring, qkv_pieces = [normed], [project(normed)]
        held = ordered(normed, wout_ring[-1])
        for step in range(1, n_tp):
            held = tp_shift(held, 1, n_tp)
            normed_ring.append(held)
            qkv_pieces.append(project(held))
            held = ordered(held, qkv_pieces[step - 1])

        wqkv_ring = [wqkv_loc]
        held = ordered(wqkv_loc, normed_ring[-1])
        for _ in range(1, n_tp):
            held = tp_shift(held, 1, n_tp)
            wqkv_ring.append(held)
            held = ordered(held, d_attn_send)
        wqkv_rest = lax.all_gather(jnp.concatenate(wqkv_ring[1:], axis=1), "fsdp", axis=0, tiled=True)

        qkv_proj = to_sequence(qkv_pieces)
        positions = jnp.arange(seq_len)
        queries, keys_rot, values = split_qkv(qkv_proj, positions, kv_loc, head_dim)
        pad_zeros = jnp.zeros((n_rows, WINDOW, kv_loc, head_dim), jnp.bfloat16)
        keys_ext = jnp.concatenate([pad_zeros, keys_rot], axis=1)
        values_ext = jnp.concatenate([pad_zeros, values], axis=1)
        attn_out, log_norm = attend_forward(queries, keys_ext, values_ext, sink_loc, 0)
        d_attn_send = ordered(d_attn_send, wqkv_ring[-1], attn_out)
        d_attn_mine = exchange(d_attn_send, n_tp)
        attn_flat = attn_out.reshape(n_rows, seq_len, out_loc)

        d_attn = to_sequence(d_attn_mine)
        bout_part = jnp.sum(grad_loc, axis=(0, 1), dtype=jnp.float32)
        grad_hop = tp_shift(ordered(grad_loc, d_attn_mine, attn_out), 1, n_tp)
        attn_mine = exchange(ordered([chunk_of(attn_flat, rank + step) for step in range(n_tp)], d_attn_mine), n_tp)
        attn_rows = jnp.stack([piece.reshape(n_rows, loc_len, n_fsdp, -1) for piece in attn_mine], axis=3).reshape(n_rows, loc_len, n_tp * out_loc)
        dq_rot, dk_ext, dv_ext, sink_part = attend_backward(queries, keys_ext, values_ext, sink_loc, 0, log_norm, d_attn.reshape(attn_out.shape))
        cos_tab, sin_tab = rope_tables(positions, head_dim)
        d_query = rope_back(dq_rot.astype(jnp.float32), cos_tab[:, None, None], sin_tab[:, None, None]).astype(jnp.bfloat16)
        d_key = rope_back(dk_ext[:, WINDOW:].astype(jnp.bfloat16).astype(jnp.float32), cos_tab[:, None], sin_tab[:, None]).astype(jnp.bfloat16)
        d_value = dv_ext[:, WINDOW:].astype(jnp.bfloat16)
        d_qkv = jnp.concatenate([d_query, d_key[:, :, :, None], d_value[:, :, :, None]], axis=3).reshape(qkv_proj.shape)

        d_ring = jnp.concatenate([chunk_of(d_qkv, rank - step) for step in range(n_tp)], axis=1)
        wqkv_part = jnp.einsum("ntd,ntc->dc", jnp.concatenate(normed_ring, axis=1), d_ring, preferred_element_type=jnp.float32)
        grad_wqkv = lax.psum_scatter(wqkv_part, "fsdp", scatter_dimension=0, tiled=True)
        grad_ring = [grad_loc, grad_hop]
        held = ordered(grad_hop, wqkv_part, attn_mine)
        for _ in range(n_tp - 2):
            held = tp_shift(held, 1, n_tp)
            grad_ring.append(held)
        attn_ring = jnp.concatenate([chunk_of(attn_flat, rank - step) for step in range(n_tp)], axis=1)
        wout_part = jnp.einsum("nth,ntk->hk", attn_ring, jnp.concatenate(grad_ring, axis=1), preferred_element_type=jnp.float32)
        grad_wout = lax.psum_scatter(wout_part, "fsdp", scatter_dimension=0, tiled=True)
        d_mine = exchange(ordered([chunk_of(d_qkv, rank + step) for step in range(n_tp)], grad_ring[-1]), n_tp)
        proj_out = jnp.dot(attn_rows, wout_all, preferred_element_type=jnp.float32)
        resid_out = (resid_f32 + proj_out + b_out.astype(jnp.float32)).astype(jnp.bfloat16)
        grad_bqkv = lax.psum(jnp.sum(d_qkv, axis=(0, 1), dtype=jnp.float32), "fsdp")
        grad_sinks = lax.psum(sink_part, "fsdp")
        d_normed = jnp.einsum("ntc,dc->ntd", d_mine[0], wqkv_own, preferred_element_type=jnp.float32) + jnp.einsum("ntc,dc->ntd", jnp.concatenate(d_mine[1:], axis=2), wqkv_rest, preferred_element_type=jnp.float32)
        grad_resid, gain_part = norm_backward(d_normed, resid_f32, inv_rms, norm_gain, grad_loc)
        grad_gain, grad_bout = lax.psum((gain_part, bout_part), ("fsdp", "tp"))
        return (resid_out, grad_resid, grad_gain, grad_wqkv, grad_bqkv, grad_sinks, grad_wout, grad_bout)

    return jax.shard_map(device_step, mesh=mesh, in_specs=in_specs, out_specs=out_specs, check_vma=False)
```

```python
import jax
import jax.numpy as jnp
from jax import lax
from jax.sharding import PartitionSpec as P


EPS = 1e-5
ROPE_BASE = 150000.0
WINDOW = 128


def rope_tables(positions, head_dim):
    inv_freq = ROPE_BASE ** (-2.0 * jnp.arange(head_dim // 2).astype(jnp.float32) / head_dim)
    angles = positions.astype(jnp.float32)[:, None] * inv_freq[None, :]
    return jnp.cos(angles), jnp.sin(angles)


def apply_rope(head_vals, cos_tab, sin_tab):
    half_dim = head_vals.shape[-1] // 2
    first_half = head_vals[..., :half_dim]
    second_half = head_vals[..., half_dim:]
    return jnp.concatenate([first_half * cos_tab - second_half * sin_tab, second_half * cos_tab + first_half * sin_tab], axis=-1)


def rope_back(head_grads, cos_tab, sin_tab):
    half_dim = head_grads.shape[-1] // 2
    first_half = head_grads[..., :half_dim]
    second_half = head_grads[..., half_dim:]
    return jnp.concatenate([first_half * cos_tab + second_half * sin_tab, second_half * cos_tab - first_half * sin_tab], axis=-1)


def split_qkv(qkv_proj, positions, kv_count, head_dim):
    n_rows, seq_len = qkv_proj.shape[0], qkv_proj.shape[1]
    grouped = qkv_proj.reshape(n_rows, seq_len, kv_count, -1, head_dim)
    group_size = grouped.shape[3] - 2
    cos_tab, sin_tab = rope_tables(positions, head_dim)
    queries = apply_rope(grouped[:, :, :, :group_size].astype(jnp.float32), cos_tab[:, None, None], sin_tab[:, None, None])
    keys_rot = apply_rope(grouped[:, :, :, group_size].astype(jnp.float32), cos_tab[:, None], sin_tab[:, None])
    return queries.astype(jnp.bfloat16), keys_rot.astype(jnp.bfloat16), grouped[:, :, :, group_size + 1]


def band_mask(first_pos, blk_start):
    q_idx = jnp.arange(WINDOW)[:, None]
    k_idx = jnp.arange(2 * WINDOW)[None, :]
    return (k_idx > q_idx) & (k_idx <= q_idx + WINDOW) & (first_pos + blk_start - WINDOW + k_idx >= 0)


def block_scores(q_blk, k_blk, first_pos, blk_start):
    qk_scale = q_blk.shape[-1] ** -0.5
    scores = jnp.einsum("niegd,njed->negij", q_blk, k_blk, preferred_element_type=jnp.float32) * qk_scale
    return jnp.where(band_mask(first_pos, blk_start), scores, -1e30)


def attend_forward(queries, keys_ext, values_ext, sink_loc, first_pos):
    n_rows, q_len, kv_loc, group_size, _ = queries.shape
    sink_col = sink_loc.reshape(1, kv_loc, group_size, 1)

    def block_body(block_idx, loop_carry):
        out_acc, norm_acc = loop_carry
        blk_start = block_idx * WINDOW
        q_blk = lax.dynamic_slice_in_dim(queries, blk_start, WINDOW, axis=1)
        k_blk = lax.dynamic_slice_in_dim(keys_ext, blk_start, 2 * WINDOW, axis=1)
        v_blk = lax.dynamic_slice_in_dim(values_ext, blk_start, 2 * WINDOW, axis=1)
        scores = block_scores(q_blk, k_blk, first_pos, blk_start)
        row_max = jnp.maximum(jnp.max(scores, axis=-1), sink_col)
        exp_scores = jnp.exp(scores - row_max[..., None])
        row_denom = jnp.sum(exp_scores, axis=-1) + jnp.exp(sink_col - row_max)
        attn_probs = (exp_scores / row_denom[..., None]).astype(jnp.bfloat16)
        out_blk = jnp.einsum("negij,njed->niegd", attn_probs, v_blk, preferred_element_type=jnp.float32)
        out_acc = lax.dynamic_update_slice_in_dim(out_acc, out_blk.astype(jnp.bfloat16), blk_start, axis=1)
        norm_acc = lax.dynamic_update_slice_in_dim(norm_acc, row_max + jnp.log(row_denom), blk_start, axis=3)
        return out_acc, norm_acc

    init_carry = (jnp.zeros(queries.shape, jnp.bfloat16), jnp.zeros((n_rows, kv_loc, group_size, q_len), jnp.float32))
    return lax.fori_loop(0, q_len // WINDOW, block_body, init_carry)


def attend_backward(queries, keys_ext, values_ext, sink_loc, first_pos, log_norm, d_out):
    _, q_len, kv_loc, group_size, head_dim = queries.shape
    qk_scale = head_dim ** -0.5
    sink_col = sink_loc.reshape(1, kv_loc, group_size, 1)

    def block_body(block_idx, loop_carry):
        dq_acc, dk_acc, dv_acc, dsink_acc = loop_carry
        blk_start = block_idx * WINDOW
        q_blk = lax.dynamic_slice_in_dim(queries, blk_start, WINDOW, axis=1)
        k_blk = lax.dynamic_slice_in_dim(keys_ext, blk_start, 2 * WINDOW, axis=1)
        v_blk = lax.dynamic_slice_in_dim(values_ext, blk_start, 2 * WINDOW, axis=1)
        do_blk = lax.dynamic_slice_in_dim(d_out, blk_start, WINDOW, axis=1)
        norm_blk = lax.dynamic_slice_in_dim(log_norm, blk_start, WINDOW, axis=3)
        attn_probs = jnp.exp(block_scores(q_blk, k_blk, first_pos, blk_start) - norm_blk[..., None])
        dv_blk = jnp.einsum("negij,niegd->njed", attn_probs.astype(jnp.bfloat16), do_blk, preferred_element_type=jnp.float32)
        d_probs = jnp.einsum("niegd,njed->negij", do_blk, v_blk, preferred_element_type=jnp.float32).astype(jnp.bfloat16).astype(jnp.float32)
        row_dot = jnp.sum(attn_probs * d_probs, axis=-1)
        d_scores = (attn_probs * (d_probs - row_dot[..., None])).astype(jnp.bfloat16)
        sink_probs = jnp.exp(sink_col - norm_blk)
        dsink_acc = dsink_acc - jnp.sum(sink_probs * row_dot, axis=(0, 3))
        dq_blk = jnp.einsum("negij,njed->niegd", d_scores, k_blk, preferred_element_type=jnp.float32) * qk_scale
        dk_blk = jnp.einsum("negij,niegd->njed", d_scores, q_blk, preferred_element_type=jnp.float32) * qk_scale
        dq_acc = lax.dynamic_update_slice_in_dim(dq_acc, dq_blk.astype(jnp.bfloat16), blk_start, axis=1)
        dk_acc = lax.dynamic_update_slice_in_dim(dk_acc, lax.dynamic_slice_in_dim(dk_acc, blk_start, 2 * WINDOW, axis=1) + dk_blk, blk_start, axis=1)
        dv_acc = lax.dynamic_update_slice_in_dim(dv_acc, lax.dynamic_slice_in_dim(dv_acc, blk_start, 2 * WINDOW, axis=1) + dv_blk, blk_start, axis=1)
        return dq_acc, dk_acc, dv_acc, dsink_acc

    init_carry = (jnp.zeros(queries.shape, jnp.bfloat16), jnp.zeros(keys_ext.shape, jnp.float32), jnp.zeros(values_ext.shape, jnp.float32), jnp.zeros((kv_loc, group_size), jnp.float32))
    dq_all, dk_all, dv_all, dsink_all = lax.fori_loop(0, q_len // WINDOW, block_body, init_carry)
    return dq_all, dk_all, dv_all, dsink_all.reshape(-1)


def norm_backward(d_normed, resid_f32, inv_rms, norm_gain, grad_loc):
    d_normed = d_normed.astype(jnp.bfloat16).astype(jnp.float32)
    gain_grad = d_normed * norm_gain
    d_resid = inv_rms * (gain_grad - resid_f32 * inv_rms * inv_rms * jnp.mean(gain_grad * resid_f32, axis=-1, keepdims=True))
    grad_resid = (grad_loc.astype(jnp.float32) + d_resid).astype(jnp.bfloat16)
    grad_gain = jnp.sum(d_normed * resid_f32 * inv_rms, axis=(0, 1))
    return grad_resid, grad_gain


def ordered(value, *earlier):
    return lax.optimization_barrier((value, earlier))[0]


def tp_shift(value, step, n_ranks):
    return lax.ppermute(value, "tp", [(rank, (rank + step) % n_ranks) for rank in range(n_ranks)])


def ring_gather(shard, n_ranks, *earlier):
    pieces = [shard]
    held = ordered(shard, *earlier) if earlier else shard
    for _ in range(n_ranks - 1):
        held = tp_shift(held, 1, n_ranks)
        pieces.append(held)
    return pieces


def exchange(pieces_by_dest, n_ranks):
    received = [pieces_by_dest[0]]
    for step in range(1, n_ranks):
        received.append(tp_shift(pieces_by_dest[step], step, n_ranks))
    return received


def solution(mesh):
    act_spec = P("fsdp", "tp", None)
    wout_spec = P(("tp", "fsdp"), None)
    in_specs = (act_spec, act_spec, P(), P("fsdp", "tp"), P("tp"), P("tp"), wout_spec, P())
    out_specs = (act_spec, act_spec, P(), P("fsdp", "tp"), P("tp"), P("tp"), wout_spec, P())
    n_tp = mesh.shape["tp"]
    n_fsdp = mesh.shape["fsdp"]

    def device_step(resid_loc, grad_loc, norm_gain, wqkv_loc, bqkv_loc, sink_loc, wout_loc, b_out):
        n_rows, loc_len, _ = resid_loc.shape
        heads_loc = sink_loc.shape[0]
        rank = lax.axis_index("tp")
        seq_len = loc_len * n_tp
        head_dim = wout_loc.shape[0] * n_fsdp // heads_loc
        kv_loc = (wqkv_loc.shape[1] // head_dim - heads_loc) // 2
        out_loc = heads_loc * head_dim

        def chunk_of(arr, owner):
            return lax.dynamic_slice_in_dim(arr, lax.rem(owner + n_tp, n_tp) * loc_len, loc_len, axis=1)

        def to_sequence(pieces):
            out = jnp.zeros((n_rows, seq_len) + pieces[0].shape[2:], pieces[0].dtype)
            for step, piece in enumerate(pieces):
                out = lax.dynamic_update_slice_in_dim(out, piece, lax.rem(rank - step + n_tp, n_tp) * loc_len, axis=1)
            return out

        resid_f32 = resid_loc.astype(jnp.float32)
        inv_rms = lax.rsqrt(jnp.mean(resid_f32 * resid_f32, axis=-1, keepdims=True) + EPS)
        normed = (resid_f32 * inv_rms * norm_gain).astype(jnp.bfloat16)

        wqkv_own = lax.all_gather(wqkv_loc, "fsdp", axis=0, tiled=True)
        wout_ring = ring_gather(wout_loc, n_tp)
        wout_all = lax.all_gather(jnp.concatenate(wout_ring, axis=0), "fsdp", axis=0, tiled=True)
        wqkv_ring = ring_gather(wqkv_loc, n_tp, wout_ring[-1])
        wqkv_rest = lax.all_gather(jnp.concatenate(wqkv_ring[1:], axis=1), "fsdp", axis=0, tiled=True)

        def project(piece):
            return (jnp.dot(piece, wqkv_own, preferred_element_type=jnp.float32) + bqkv_loc.astype(jnp.float32)).astype(jnp.bfloat16)

        d_attn_rows = jnp.einsum("ntk,hk->nth", grad_loc, wout_all, preferred_element_type=jnp.float32).astype(jnp.bfloat16).reshape(n_rows, loc_len, n_fsdp, n_tp, -1)
        d_attn_send = [d_attn_rows[:, :, :, (n_tp - step) % n_tp].reshape(n_rows, loc_len, out_loc) for step in range(n_tp)]

        normed_ring, qkv_pieces = [normed], [project(normed)]
        held = ordered(normed, wqkv_ring[-1])
        for step in range(1, n_tp):
            held = tp_shift(held, 1, n_tp)
            normed_ring.append(held)
            qkv_pieces.append(project(held))
            held = ordered(held, qkv_pieces[step - 1], d_attn_send) if step == n_tp - 2 else ordered(held, qkv_pieces[step - 1])

        d_attn_send = ordered(d_attn_send, normed_ring[-1])
        d_attn_mine = exchange(d_attn_send, n_tp)
        qkv_proj = to_sequence(qkv_pieces)
        positions = jnp.arange(seq_len)
        queries, keys_rot, values = split_qkv(qkv_proj, positions, kv_loc, head_dim)
        pad_zeros = jnp.zeros((n_rows, WINDOW, kv_loc, head_dim), jnp.bfloat16)
        keys_ext = jnp.concatenate([pad_zeros, keys_rot], axis=1)
        values_ext = jnp.concatenate([pad_zeros, values], axis=1)
        attn_out, log_norm = attend_forward(queries, keys_ext, values_ext, sink_loc, 0)
        attn_flat = attn_out.reshape(n_rows, seq_len, out_loc)

        d_attn = to_sequence(d_attn_mine)
        bout_part = jnp.sum(grad_loc, axis=(0, 1), dtype=jnp.float32)
        grad_hop = tp_shift(ordered(grad_loc, d_attn_mine, attn_out), 1, n_tp)
        attn_mine = exchange(ordered([chunk_of(attn_flat, rank + step) for step in range(n_tp)], d_attn_mine), n_tp)
        attn_rows = jnp.stack([piece.reshape(n_rows, loc_len, n_fsdp, -1) for piece in attn_mine], axis=3).reshape(n_rows, loc_len, n_tp * out_loc)
        dq_rot, dk_ext, dv_ext, sink_part = attend_backward(queries, keys_ext, values_ext, sink_loc, 0, log_norm, d_attn.reshape(attn_out.shape))
        cos_tab, sin_tab = rope_tables(positions, head_dim)
        d_query = rope_back(dq_rot.astype(jnp.float32), cos_tab[:, None, None], sin_tab[:, None, None]).astype(jnp.bfloat16)
        d_key = rope_back(dk_ext[:, WINDOW:].astype(jnp.bfloat16).astype(jnp.float32), cos_tab[:, None], sin_tab[:, None]).astype(jnp.bfloat16)
        d_value = dv_ext[:, WINDOW:].astype(jnp.bfloat16)
        d_qkv = jnp.concatenate([d_query, d_key[:, :, :, None], d_value[:, :, :, None]], axis=3).reshape(qkv_proj.shape)

        d_ring = jnp.concatenate([chunk_of(d_qkv, rank - step) for step in range(n_tp)], axis=1)
        wqkv_part = jnp.einsum("ntd,ntc->dc", jnp.concatenate(normed_ring, axis=1), d_ring, preferred_element_type=jnp.float32)
        grad_wqkv = lax.psum_scatter(wqkv_part, "fsdp", scatter_dimension=0, tiled=True)
        grad_ring = [grad_loc, grad_hop]
        grad_bqkv, grad_sinks = lax.psum((jnp.sum(d_qkv, axis=(0, 1), dtype=jnp.float32), sink_part), "fsdp")
        held = ordered(grad_hop, wqkv_part, attn_mine)
        for _ in range(2, n_tp):
            held = tp_shift(held, 1, n_tp)
            grad_ring.append(held)
            held = ordered(held, grad_bqkv, grad_sinks)
        attn_ring = jnp.concatenate([chunk_of(attn_flat, rank - step) for step in range(n_tp)], axis=1)
        wout_part = jnp.einsum("nth,ntk->hk", attn_ring, jnp.concatenate(grad_ring, axis=1), preferred_element_type=jnp.float32)
        grad_wout = lax.psum_scatter(wout_part, "fsdp", scatter_dimension=0, tiled=True)
        d_mine = exchange(ordered([chunk_of(d_qkv, rank + step) for step in range(n_tp)], wout_part), n_tp)
        proj_out = jnp.dot(attn_rows, wout_all, preferred_element_type=jnp.float32)
        resid_out = (resid_f32 + proj_out + b_out.astype(jnp.float32)).astype(jnp.bfloat16)
        d_normed = jnp.einsum("ntc,dc->ntd", d_mine[0], wqkv_own, preferred_element_type=jnp.float32)
        d_normed = d_normed + jnp.einsum("ntc,dc->ntd", jnp.concatenate(d_mine[1:], axis=2), wqkv_rest, preferred_element_type=jnp.float32)
        grad_resid, gain_part = norm_backward(d_normed, resid_f32, inv_rms, norm_gain, grad_loc)
        grad_gain, grad_bout = lax.psum((gain_part, bout_part), ("fsdp", "tp"))
        return (resid_out, grad_resid, grad_gain, grad_wqkv, grad_bqkv, grad_sinks, grad_wout, grad_bout)

    return jax.shard_map(device_step, mesh=mesh, in_specs=in_specs, out_specs=out_specs, check_vma=False)
```
